8 devices in a mesh: data: 8 (over z, y, x, core).
Axes of the slice: x: 2, y: 2, z: 1, core: 2. Of those that a mesh axis runs over, the one named last changes fastest.
Arguments:
- w_one: float32 [8, 1024, 4096], P(None, 'data')
- w_two: float32 [8, 4096, 1024], P(None, 'data')
- mom_one: float32 [8, 1024, 4096], P(None, 'data')
- mom_two: float32 [8, 4096, 1024], P(None, 'data')
- x_zero: bfloat16 [16384, 1024], P('data')
- y_zero: bfloat16 [16384, 1024], P('data')
- x_one: bfloat16 [16384, 1024], P('data')
- y_one: bfloat16 [16384, 1024], P('data')
Outputs:
- output 1: float32 [8, 1024, 4096], P(None, 'data')
- output 2: float32 [8, 4096, 1024], P(None, 'data')
- output 3: float32 [8, 1024, 4096], P(None, 'data')
- output 4: float32 [8, 4096, 1024], P(None, 'data')
- output 5: float32 [16384], P('data')
- output 6: float32 [16384, 1024], P('data')
All inputs are finite; a program needn't handle non-finite values.
Results may differ from the reference program's by a relative error of at most 0.00842355.
Values are sent between devices in bfloat16 or wider.
A program may use at most 1 GiB of HBM per device.

```python
import jax
import jax.numpy as jnp
from jax import lax

DATA_DEVS = 8
TOK_DEV = 2048
LAYERS = 8
D_MODEL = 1024
D_FF = 4096

BATCH = DATA_DEVS * TOK_DEV
LEARN_RATE = 0.1
MOMENTUM = 0.9


def draw_rows(key_vals, key_shift, centre, spread):
    base_vals = jax.random.normal(key_vals, (DATA_DEVS, TOK_DEV, D_MODEL), jnp.float32)
    col_shift = jax.random.normal(key_shift, (DATA_DEVS, 1, D_MODEL), jnp.float32)
    return (spread * base_vals + centre + 0.5 * col_shift).reshape(BATCH, D_MODEL).astype(jnp.bfloat16)


def setup_inputs(seed: int = 0) -> dict:
    key_list = jax.random.split(jax.random.key(seed), 16)
    w_one = jax.random.normal(key_list[0], (LAYERS, D_MODEL, D_FF), jnp.float32) * D_MODEL ** -0.5
    w_two = jax.random.normal(key_list[1], (LAYERS, D_FF, D_MODEL), jnp.float32) * (D_FF * LAYERS) ** -0.5
    scale_one = 0.3 * (D_MODEL * D_FF * LAYERS) ** -0.5
    row_one = 1.0 + 0.5 * jax.random.normal(key_list[2], (LAYERS, D_MODEL, 1), jnp.float32)
    col_one = jax.random.normal(key_list[3], (LAYERS, 1, D_FF), jnp.float32)
    mom_one = scale_one * (row_one * col_one + 0.5 * jax.random.normal(key_list[4], (LAYERS, D_MODEL, D_FF), jnp.float32))
    scale_two = 0.3 / D_MODEL
    row_two = 1.0 + 0.5 * jax.random.normal(key_list[5], (LAYERS, D_FF, 1), jnp.float32)
    col_two = jax.random.normal(key_list[6], (LAYERS, 1, D_MODEL), jnp.float32)
    mom_two = scale_two * (row_two * col_two + 0.5 * jax.random.normal(key_list[7], (LAYERS, D_FF, D_MODEL), jnp.float32))
    return {
        "w_one": w_one,
        "w_two": w_two,
        "mom_one": mom_one,
        "mom_two": mom_two,
        "x_zero": draw_rows(key_list[8], key_list[9], 0.6, 0.8),
        "y_zero": draw_rows(key_list[10], key_list[11], -0.5, 0.5),
        "x_one": draw_rows(key_list[12], key_list[13], 0.6, 0.8),
        "y_one": draw_rows(key_list[14], key_list[15], -0.5, 0.5),
    }


def run_stack(w_one_b, w_two_b, h_start):
    def layer_step(h_cur, weights):
        w_in, w_out = weights
        act_in = h_cur.astype(jnp.bfloat16)
        pre_act = jnp.dot(act_in, w_in, preferred_element_type=jnp.float32)
        hidden = jax.nn.gelu(pre_act).astype(jnp.bfloat16)
        h_next = h_cur + jnp.dot(hidden, w_out, preferred_element_type=jnp.float32)
        return h_next, (act_in, pre_act, hidden)
    return lax.scan(layer_step, h_start, (w_one_b, w_two_b))


def local_grads(w_one_b, w_two_b, x_rows, y_rows):
    h_end, saved_vals = run_stack(w_one_b, w_two_b, x_rows.astype(jnp.float32))
    d_start = (h_end - y_rows.astype(jnp.float32)) / (BATCH * D_MODEL)

    def back_step(d_state, layer_vals):
        w_in, w_out, act_in, pre_act, hidden = layer_vals
        d_low = d_state.astype(jnp.bfloat16)
        grad_out = jnp.dot(hidden.T, d_low, preferred_element_type=jnp.float32).astype(jnp.bfloat16)
        d_hidden = jnp.dot(d_low, w_out.T, preferred_element_type=jnp.float32)
        d_pre = jax.vjp(jax.nn.gelu, pre_act)[1](d_hidden)[0].astype(jnp.bfloat16)
        grad_in = jnp.dot(act_in.T, d_pre, preferred_element_type=jnp.float32).astype(jnp.bfloat16)
        d_next = d_state + jnp.dot(d_pre, w_in.T, preferred_element_type=jnp.float32)
        return d_next, (grad_in, grad_out)

    act_ins, pre_acts, hiddens = saved_vals
    return lax.scan(back_step, d_start, (w_one_b, w_two_b, act_ins, pre_acts, hiddens), reverse=True)[1]


def reference(w_one, w_two, mom_one, mom_two, x_zero, y_zero, x_one, y_one):
    w_one_b = w_one.astype(jnp.bfloat16)
    w_two_b = w_two.astype(jnp.bfloat16)
    x_dev = x_zero.reshape(DATA_DEVS, TOK_DEV, D_MODEL)
    y_dev = y_zero.reshape(DATA_DEVS, TOK_DEV, D_MODEL)

    def add_device(acc_pair, row_pair):
        grad_in, grad_out = local_grads(w_one_b, w_two_b, row_pair[0], row_pair[1])
        return (acc_pair[0] + grad_in.astype(jnp.float32), acc_pair[1] + grad_out.astype(jnp.float32)), None

    zeros_pair = (jnp.zeros(w_one.shape, jnp.float32), jnp.zeros(w_two.shape, jnp.float32))
    grad_sums = lax.scan(add_device, zeros_pair, (x_dev, y_dev))[0]
    new_mom_one = MOMENTUM * mom_one + grad_sums[0].astype(jnp.bfloat16).astype(jnp.float32)
    new_mom_two = MOMENTUM * mom_two + grad_sums[1].astype(jnp.bfloat16).astype(jnp.float32)
    new_w_one = w_one - LEARN_RATE * new_mom_one
    new_w_two = w_two - LEARN_RATE * new_mom_two
    next_one_b = new_w_one.astype(jnp.bfloat16)
    next_two_b = new_w_two.astype(jnp.bfloat16)

    def device_forward(x_rows):
        return run_stack(next_one_b, next_two_b, x_rows.astype(jnp.float32))[0]

    h_last = lax.map(device_forward, x_one.reshape(DATA_DEVS, TOK_DEV, D_MODEL)).reshape(BATCH, D_MODEL)
    loss_rows = jnp.sum(jnp.square(h_last - y_one.astype(jnp.float32)), axis=1) / (2 * D_MODEL)
    return new_w_one, new_w_two, new_mom_one, new_mom_two, loss_rows, h_last
```

```python
import functools

import jax
import jax.numpy as jnp
from jax import lax
from jax.experimental import pallas as pl
from jax.experimental.pallas import tpu as pltpu
from jax.sharding import PartitionSpec as P

BF16, F32 = jnp.bfloat16, jnp.float32
LEARN_RATE = 0.1
MOMENTUM = 0.9
GELU_C = 0.7978845608028654
GELU_A = 0.044715
VMEM_LIMIT = 60 * 1024 * 1024
ROW_TILE = 256
CORE, CHIP_X, CHIP_Y = 1, 2, 4


def after(value, dep):
    return lax.optimization_barrier((value, dep))[0]


def swap(value, bit):
    return lax.ppermute(value, "data", [(i, i ^ bit) for i in range(8)])


def call_params():
    return pltpu.CompilerParams(dimension_semantics=("arbitrary",), vmem_limit_bytes=VMEM_LIMIT)


def matmul_cost(products, nbytes):
    return pl.CostEstimate(flops=int(products * 2 * 2048 * 1024 * 4096), bytes_accessed=nbytes, transcendentals=0)


def gelu_tanh(u):
    u2 = u * u
    return jnp.tanh(u * (GELU_C + (GELU_C * GELU_A) * u2)), u2


def gelu(u):
    t, _ = gelu_tanh(u)
    half = 0.5 * u
    return half + half * t


def gelu_slope(u):
    t, u2 = gelu_tanh(u)
    return 0.5 + 0.5 * t + (0.5 * u) * (1.0 - t * t) * (GELU_C + (3.0 * GELU_C * GELU_A) * u2)


def dot(a, b, dims):
    return lax.dot_general(a, b, ((dims[:1], dims[1:]), ((), ())), preferred_element_type=F32)


def w_in_block(w_ref, c):
    return w_ref[0, :, 0, c * 128 : (c + 1) * 128, :].reshape(1024, 1024)


def w_out_block(w_ref, c):
    return w_ref[0, 2 * c : 2 * c + 2, 0].reshape(1024, 1024)


def weight_specs(k):
    once = pl.Buffered(1)
    return [
        pl.BlockSpec((1, 8, 1, 512, 1024), lambda i: (k, 0, 0, 0, 0), pipeline_mode=once),
        pl.BlockSpec((1, 8, 1, 512, 1024), lambda i: (k, 0, 1, 0, 0), pipeline_mode=once),
    ]


def pack_kernel(w_one_ref, w_two_ref, o_ref):
    for c in range(4):
        o_ref[0, c * 128 : (c + 1) * 128, :] = w_one_ref[0, :, c * 1024 : (c + 1) * 1024].astype(BF16)
    o_ref[0, 512:, :] = w_two_ref[0].astype(BF16)


def pack_weights(w_one, w_two, lo, hi):
    return pl.pallas_call(
        pack_kernel,
        grid=(hi - lo,),
        in_specs=[
            pl.BlockSpec((1, 128, 4096), lambda i: (lo + i, 0, 0)),
            pl.BlockSpec((1, 512, 1024), lambda i: (lo + i, 0, 0)),
        ],
        out_specs=pl.BlockSpec((1, 1024, 1024), lambda i: (i, 0, 0)),
        out_shape=jax.ShapeDtypeStruct((hi - lo, 1024, 1024), BF16),
        compiler_params=call_params(),
        cost_estimate=matmul_cost(0.1, 6 * 2**20),
        name="pack_weights",
    )(w_one, w_two)


def fwd_kernel(keep, h_ref, w_one_ref, w_two_ref, hn_ref, *saved_refs):
    h = h_ref[...]
    a = h.astype(BF16)
    hidden = []
    for c in range(4):
        u = dot(a, w_in_block(w_one_ref, c), (1, 0))
        z = gelu(u).astype(BF16)
        hidden.append(z)
        if keep:
            saved_refs[1][:, c * 1024 : (c + 1) * 1024] = u
            saved_refs[2][:, c * 1024 : (c + 1) * 1024] = z
    if keep:
        saved_refs[0][...] = a
    z = jnp.concatenate(hidden, axis=1)
    hn_ref[...] = h + dot(z, w_two_ref[0, :, 0].reshape(4096, 1024), (1, 0))


def layer_fwd(h, w_all, k, keep, ROW_TILE=ROW_TILE):
    n, d = h.shape
    row = lambda i: (i, 0)
    widths = [(d, F32)] + ([(d, BF16), (4096, F32), (4096, BF16)] if keep else [])
    return pl.pallas_call(
        functools.partial(fwd_kernel, keep),
        grid=(n // ROW_TILE,),
        in_specs=[pl.BlockSpec((ROW_TILE, d), row)] + weight_specs(k),
        out_specs=[pl.BlockSpec((ROW_TILE, width), row) for width, _ in widths],
        out_shape=[jax.ShapeDtypeStruct((n, width), dtype) for width, dtype in widths],
        compiler_params=call_params(),
        cost_estimate=matmul_cost(2.6, 80 * 2**20),
        name="layer_fwd",
    )(h, w_all, w_all)


def bwd_kernel(last, d_ref, dl_ref, u_ref, w_one_ref, w_two_ref, r_ref, *next_refs):
    q = dot(dl_ref[...], w_two_ref[0, :, 0].reshape(4096, 1024), (1, 1))
    r = (gelu_slope(u_ref[...]) * q).astype(BF16)
    r_ref[...] = r
    if not last:
        w_in = jnp.concatenate([w_in_block(w_one_ref, c) for c in range(4)], axis=1)
        total = d_ref[...] + dot(r, w_in, (1, 1))
        next_refs[0][...] = total
        next_refs[1][...] = total.astype(BF16)


def layer_bwd(d, d_low, u, w_all, k, last, ROW_TILE=ROW_TILE):
    n, dm = d.shape
    row = lambda i: (i, 0)
    widths = [(4096, BF16)] + ([] if last else [(dm, F32), (dm, BF16)])
    return pl.pallas_call(
        functools.partial(bwd_kernel, last),
        grid=(n // ROW_TILE,),
        in_specs=[pl.BlockSpec((ROW_TILE, dm), row), pl.BlockSpec((ROW_TILE, dm), row), pl.BlockSpec((ROW_TILE, 4096), row)] + weight_specs(k),
        out_specs=[pl.BlockSpec((ROW_TILE, width), row) for width, _ in widths],
        out_shape=[jax.ShapeDtypeStruct((n, width), dtype) for width, dtype in widths],
        compiler_params=call_params(),
        cost_estimate=matmul_cost(2.8, 80 * 2**20),
        name="layer_bwd",
    )(d, d_low, u, w_all, w_all)


def grad_kernel(keep, idx_ref, l0, l1, l2, l3, rhs_ref, *refs):
    lhs = jnp.concatenate([l0[...], l1[...], l2[...], l3[...]], axis=1)
    grad = dot(lhs, rhs_ref[...], (0, 0)).astype(BF16).reshape(4, 128, 1024)
    if not keep:
        refs[0][...] = grad
        return
    recv_ref, xa_ref, yb_ref, ka_ref, kb_ref = refs
    grad = (grad.astype(F32) + recv_ref[...].astype(F32)).astype(BF16)
    step = pl.program_id(0)

    @pl.when(step < 2)
    def _():
        xa_ref[0] = grad[1]
        xa_ref[1] = grad[3]
        ka_ref[0] = grad[0]
        ka_ref[1] = grad[2]

    @pl.when(step >= 2)
    def _():
        yb_ref[0] = grad[2]
        yb_ref[1] = grad[3]
        kb_ref[0] = grad[0]
        kb_ref[1] = grad[1]


def grad_call(which, idx, lhs, rhs, recv=None):
    n = lhs.shape[0]
    keep = recv is not None
    if which == 1:
        full, half = (4, 128, 4096), (2, 128, 2048)
        lhs_maps = [functools.partial(lambda m, j, idx: (0, idx[m]), m) for m in range(4)]
        rhs_map = lambda j, idx: (0, j)
        at = lambda pos: (0, 0, pos)
    else:
        full, half = (4, 512, 1024), (2, 256, 1024)
        lhs_maps = [functools.partial(lambda m, j, idx: (0, idx[m] * 4 + j), m) for m in range(4)]
        rhs_map = lambda j, idx: (0, 0)
        at = lambda pos: (0, pos, 0)
    full_spec = pl.BlockSpec((4, 128, 1024), lambda j, idx: at(j))
    first = pl.BlockSpec((2, 128, 1024), lambda j, idx: at(jnp.minimum(j, 1)))
    second = pl.BlockSpec((2, 128, 1024), lambda j, idx: at(jnp.maximum(j - 2, 0)))
    shape = lambda s: jax.ShapeDtypeStruct(s, BF16)
    out = pl.pallas_call(
        functools.partial(grad_kernel, keep),
        grid_spec=pltpu.PrefetchScalarGridSpec(
            num_scalar_prefetch=1,
            grid=(4,),
            in_specs=[pl.BlockSpec((n, 128), lhs_map) for lhs_map in lhs_maps]
            + [pl.BlockSpec((n, 1024), rhs_map)]
            + ([full_spec] if keep else []),
            out_specs=[first, second, first, second] if keep else full_spec,
        ),
        out_shape=[shape(half)] * 4 if keep else shape(full),
        compiler_params=call_params(),
        cost_estimate=matmul_cost(0.7, 20 * 2**20),
        name="grad_keep" if keep else "grad_send",
    )(idx, lhs, lhs, lhs, lhs, rhs, *([recv] if keep else []))
    return out


def first_exchange(xa, yb, ka, kb):
    return ka, swap(xa, CHIP_X), kb, swap(yb, CHIP_Y)


def middle_kernel(*refs):
    for i in range(4):
        refs[8 + i][...] = (refs[2 * i][...].astype(F32) + refs[2 * i + 1][...].astype(F32)).astype(BF16)


def second_exchange(one, two):
    args = one + two
    spec_one = pl.BlockSpec((1, 128, 2048), lambda i: (1, 0, 0))
    spec_two = pl.BlockSpec((1, 256, 1024), lambda i: (1, 0, 0))
    out_one = pl.BlockSpec((1, 128, 2048), lambda i: (0, 0, 0))
    out_two = pl.BlockSpec((1, 256, 1024), lambda i: (0, 0, 0))
    sums = pl.pallas_call(
        middle_kernel,
        grid=(1,),
        in_specs=[spec_one] * 4 + [spec_two] * 4,
        out_specs=[out_one] * 2 + [out_two] * 2,
        out_shape=[jax.ShapeDtypeStruct((1, 128, 2048), BF16)] * 2 + [jax.ShapeDtypeStruct((1, 256, 1024), BF16)] * 2,
        compiler_params=call_params(),
        cost_estimate=matmul_cost(0.15, 6 * 2**20),
        name="middle_sum",
    )(*args)

    terms = []
    for (ka, rxa, kb, ryb), (sum_a, sum_b) in ((one, sums[:2]), (two, sums[2:])):
        terms.append([ka, rxa, swap(sum_a, CHIP_Y), kb, ryb, swap(sum_b, CHIP_X)])
    return sums, terms


def update_kernel(n_alias, *refs):
    w_refs, m_refs = refs[0:2], refs[2:4]
    terms = (refs[4:10], refs[10:16])
    nw_refs, nm_refs, wb_ref = refs[16 + n_alias : 18 + n_alias], refs[18 + n_alias : 20 + n_alias], refs[20 + n_alias]
    step = pl.program_id(0)
    for half in range(2):

        @pl.when(step == half)
        def _():
            for i in range(2):
                t0, t1, t2 = terms[i][3 * half : 3 * half + 3]
                total = (t0[0].astype(F32) + t1[0].astype(F32)) + t2[0].astype(F32)
                mom = MOMENTUM * m_refs[i][0] + total.astype(BF16).astype(F32)
                new_w = w_refs[i][0] - LEARN_RATE * mom
                nm_refs[i][0] = mom
                nw_refs[i][0] = new_w
                low = new_w.astype(BF16)
                if i == 0:
                    for c in range(2):
                        row = half * 256 + c * 128
                        wb_ref[0, row : row + 128, :] = low[:, c * 1024 : (c + 1) * 1024]
                else:
                    row = 512 + half * 256
                    wb_ref[0, row : row + 256, :] = low


def update_layer(layer, w_one, w_two, m_one, m_two, terms_one, terms_two, carried):
    shapes = (w_one.shape, w_two.shape)
    one = pl.BlockSpec((1, 128, 2048), lambda i: (layer, 0, i))
    two = pl.BlockSpec((1, 256, 1024), lambda i: (layer, i, 0))
    term_one = pl.BlockSpec((1, 128, 2048), lambda i: (0, 0, 0))
    term_two = pl.BlockSpec((1, 256, 1024), lambda i: (0, 0, 0))
    n_alias = 0 if carried is None else 4
    outs = pl.pallas_call(
        functools.partial(update_kernel, n_alias),
        grid=(2,),
        in_specs=[one, two, one, two] + [term_one] * 6 + [term_two] * 6 + [pl.BlockSpec(memory_space=pl.ANY)] * n_alias,
        out_specs=[one, two, one, two, pl.BlockSpec((1, 1024, 1024), lambda i: (0, 0, 0))],
        out_shape=[jax.ShapeDtypeStruct(shapes[i % 2], F32) for i in range(4)] + [jax.ShapeDtypeStruct((1, 1024, 1024), BF16)],
        input_output_aliases={16 + i: i for i in range(n_alias)},
        compiler_params=call_params(),
        cost_estimate=matmul_cost(0.3, 24 * 2**20),
        name="update_layer",
    )(w_one, w_two, m_one, m_two, *terms_one, *terms_two, *(carried or ()))
    return outs[:4], outs[4]


def collect(packed):
    full = lax.all_gather(packed, "data", axis=1, tiled=True)
    return full.reshape(packed.shape[0], 8, 2, 512, 1024)


def solution(mesh):
    n_dev = mesh.shape["data"]
    w_spec = P(None, "data", None)
    row_spec = P("data", None)

    def device_step(w_one, w_two, mom_one, mom_two, x_zero, y_zero, x_one, y_one):
        layers = w_one.shape[0]
        tok_dev, d_model = x_zero.shape
        me = lax.axis_index("data")
        entries = jnp.arange(4, dtype=jnp.int32)
        keep_idx = (((me // 2) ^ entries) * 2 + me % 2).astype(jnp.int32)
        send_idx = (((me // 2) ^ entries) * 2 + 1 - me % 2).astype(jnp.int32)

        groups = [(0, 2), (2, 5), (5, 7), (7, 8)]
        packed = [pack_weights(w_one, w_two, lo, hi) for lo, hi in groups]
        gathered = [collect(packed[0]), collect(packed[1])]
        h = x_zero.astype(F32)
        weights, saved = [], []
        for g, (lo, hi) in enumerate(groups):
            for k in range(hi - lo):
                h, act_in, pre_act, hidden = layer_fwd(h, gathered[g], k, True)
                weights.append((gathered[g], k))
                saved.append((act_in, pre_act, hidden))
            if g + 2 < len(groups):
                gathered.append(collect(after(packed[g + 2], h)))

        d = (h - y_zero.astype(F32)) / (n_dev * tok_dev * d_model)
        d_low = d.astype(BF16)
        next_w = {}
        low_w = [None] * layers
        carried, pending = None, None
        early = (7, 6, 5, 3)

        def gather_next(layer, behind=None):
            part = low_w[layer]
            next_w[layer] = collect(part if behind is None else after(part, next_w[behind]))

        def update(layer, terms, carried):
            return update_layer(layer, w_one, w_two, mom_one, mom_two, terms[0], terms[1], carried)

        for layer in reversed(range(layers)):
            act_in, pre_act, hidden = saved[layer]
            w_all, k = weights[layer]
            if layer + 3 in early:
                d, d_low = after((d, d_low), next_w[layer + 3])
            send_two = grad_call(2, send_idx, hidden, d_low)
            recv_two = swap(send_two, CORE)
            outs = layer_bwd(d, after(d_low, send_two), pre_act, w_all, k, layer == 0)
            r = outs[0]
            terms = None
            if pending is not None:
                pending = after(pending, r)
                sums, terms = second_exchange(*pending)
                r = after(r, sums[0])
            send_one = grad_call(1, send_idx, act_in, r)
            recv_one = swap(send_one, CORE)
            keep_two = grad_call(2, keep_idx, hidden, after(d_low, send_one), recv_two)
            if layer == 0:
                carried, low_w[1] = update(1, terms, carried)
                keep_two = after(keep_two, low_w[1])
                gather_next(1, 3)
            keep_one = grad_call(1, keep_idx, act_in, after(r, keep_two[0]), recv_one)
            pending = (first_exchange(*keep_one), first_exchange(*keep_two))
            if layer > 0:
                d, d_low = after((outs[1], outs[2]), keep_one[0])
                if terms is not None:
                    carried, low_w[layer + 1] = update(layer + 1, after(terms, keep_one[0]), carried)
                    d, d_low = after((d, d_low), low_w[layer + 1])
                    if layer + 1 in early:
                        gather_next(layer + 1)
        sums, terms = second_exchange(*pending)
        carried, low_w[0] = update(0, terms, carried)
        gather_next(0, 1)
        gather_next(2, 0)

        h = x_one.astype(F32)
        for layer in range(layers):
            (h,) = layer_fwd(h, next_w[layer], 0, False)
            if layer == 0:
                low_w[4] = after(low_w[4], h)
                gather_next(4)
        loss_rows = jnp.sum(jnp.square(h - y_one.astype(F32)), axis=1) / (2 * d_model)
        return carried[0], carried[1], carried[2], carried[3], loss_rows, h

    return jax.shard_map(device_step, mesh=mesh, in_specs=(w_spec, w_spec, w_spec, w_spec, row_spec, row_spec, row_spec, row_spec), out_specs=(w_spec, w_spec, w_spec, w_spec, P("data"), row_spec), check_vma=False)
```
